256 devices in a mesh: expert: 64 (over z_hi, y, x), shard: 4 (over z_lo, core).
Axes of the slice: x: 4, y: 4, z: 8 (z_hi: 4, z_lo: 2; z = z_hi * 2 + z_lo), core: 2. Of those that a mesh axis runs over, the one named last changes fastest.
Arguments:
- w_gate: float32 [64, 2048, 1024], P('expert', 'shard'), may hold values from -0.1875 to 0.1875
- avg_gate: float32 [64, 2048, 1024], P('expert', 'shard'), may hold values from -0.125 to 0.125
- w_up: float32 [64, 2048, 1024], P('expert', 'shard'), may hold values from -0.1875 to 0.1875
- avg_up: float32 [64, 2048, 1024], P('expert', 'shard'), may hold values from -0.125 to 0.125
- mix_share: float32 [64], P('expert'), may hold values from 0.2 to 0.8
- router_weight: float32 [2048, 64], P('shard', 'expert'), may hold values from -0.125 to 0.125
- router_gain: float32 [2048], P('shard'), may hold values from 0.25 to 1.75
Outputs:
- serve_gate: bfloat16 [64, 2048, 1024], P('expert')
- serve_up: bfloat16 [64, 2048, 1024], P('expert')
- scale_gate: float32 [64, 1024], P('expert')
- scale_up: float32 [64, 1024], P('expert')
- serve_router: bfloat16 [2048, 64], replicated
The draws below stay inside these ranges and needn't reach their ends.
All inputs are finite; a program needn't handle non-finite values.
Results may differ from the reference program's by a relative error of at most 0.001.
Values may be sent and summed in bfloat16 or wider, within the bound.
No kernel may reach another device: no remote copies, remote signals or barrier semaphores. Data moves between devices by JAX's collectives and lax.ppermute only.
A program may use at most 64 MiB of HBM per device.

```python
import jax
import jax.numpy as jnp
from jax import lax

EXPERTS = 64
D_MODEL = 2048
D_EXPERT = 1024


def with_spikes(result, own_key, source, target, parts, factor):
    def block_of(position):
        return (jnp.arange(result.shape[position]) // (result.shape[position] // parts)).reshape((-1,) + (1,) * (result.ndim - 1 - position))

    first = jax.random.permutation(own_key, parts)[block_of(target)]
    second = (block_of(target) + parts // 2) % parts
    return jnp.where((block_of(source) == first) | (block_of(source) == second), factor * result, result)


def level_of(stream_key, dims, shards, low, top_value):
    def one(dim, parts):
        steps = jax.random.uniform(jax.random.fold_in(jax.random.fold_in(stream_key, 6), dim), (parts,), jnp.float32, low / len(shards), top_value / len(shards))
        return jnp.repeat(jnp.exp(steps), dims[dim] // parts).reshape((-1,) + (1,) * (len(dims) - dim - 1))

    gain = one(*shards[0])
    for cut in shards[1:]:
        gain = gain * one(*cut)
    return gain


def normal_values(own_key, extent, width, reach, pieces=(), kind=jnp.bfloat16):
    level = level_of(own_key, extent, pieces, -0.22, 0.18) if pieces else 1.0
    values = jax.random.normal(own_key, extent, jnp.float32) * width * level
    return jnp.minimum(jnp.maximum(values, -reach), reach).astype(kind)


def noise_with(stream_key, extent, scale, bound, shards, heavy, dtype=jnp.bfloat16):
    values = scale * jax.random.normal(stream_key, extent, jnp.float32)
    if shards:
        values = values * level_of(stream_key, extent, shards, -0.22, 0.18)
    return jnp.clip(with_spikes(values, jax.random.fold_in(stream_key, 3), *heavy), -bound, bound).astype(dtype)


def setup_inputs(seed: int = 0) -> dict:
    key_of = jax.random.split(jax.random.key(seed), 8)
    return {
        "w_gate": noise_with(key_of[0], (EXPERTS, D_MODEL, D_EXPERT), D_MODEL ** -0.5, 0.1875, ((0, 64), (1, 4)), (1, 2, 4, 2.0), jnp.float32),
        "avg_gate": normal_values(key_of[1], (EXPERTS, D_MODEL, D_EXPERT), D_MODEL ** -0.5, 0.125, ((0, 64), (1, 4)), jnp.float32),
        "w_up": noise_with(key_of[2], (EXPERTS, D_MODEL, D_EXPERT), D_MODEL ** -0.5, 0.1875, ((0, 64), (1, 4)), (1, 2, 4, 2.0), jnp.float32),
        "avg_up": normal_values(key_of[3], (EXPERTS, D_MODEL, D_EXPERT), D_MODEL ** -0.5, 0.125, ((0, 64), (1, 4)), jnp.float32),
        "mix_share": jnp.clip(0.2 + 0.6 * jax.random.uniform(key_of[4], (EXPERTS,), jnp.float32) ** level_of(key_of[4], (EXPERTS,), ((0, 64),), -0.2, 0.2), 0.2, 0.8),
        "router_weight": normal_values(key_of[5], (D_MODEL, EXPERTS), D_MODEL ** -0.5, 0.125, ((0, 4), (1, 64)), jnp.float32),
        "router_gain": jnp.clip(1.0 + 0.15 * jax.random.normal(key_of[6], (D_MODEL,), jnp.float32), 0.25, 1.75),
    }


def reference(w_gate, avg_gate, w_up, avg_up, mix_share, router_weight, router_gain):
    fresh_gate = mix_share[:, None, None] * w_gate + (1.0 - mix_share[:, None, None]) * avg_gate
    fresh_up = mix_share[:, None, None] * w_up + (1.0 - mix_share[:, None, None]) * avg_up
    scale_gate = jnp.sqrt(lax.optimization_barrier(jnp.sum(fresh_gate * fresh_gate, axis=1)))
    serve_gate = (fresh_gate / jnp.expand_dims(scale_gate, 1)).astype(jnp.bfloat16)
    scale_up = jnp.sqrt(lax.optimization_barrier(jnp.sum(fresh_up * fresh_up, axis=1)))
    serve_up = (fresh_up / jnp.expand_dims(scale_up, 1)).astype(jnp.bfloat16)
    serve_router = (router_weight * router_gain[:, None]).astype(jnp.bfloat16)
    return (serve_gate, serve_up, scale_gate, scale_up, serve_router)
```

```python
import jax
import jax.numpy as jnp
from jax import lax
from jax.sharding import PartitionSpec as P


PIECES = 2


def swap(x, axis, mask):
    n = lax.axis_size(axis)
    return lax.ppermute(x, axis, [(i, i ^ mask) for i in range(n)])


CORE, CHIP = 1, 2


def scales(fresh):
    own = jnp.sum(fresh * fresh, axis=1)
    core, chip, both = (swap(own, "shard", m) for m in (CORE, CHIP, CORE | CHIP))
    return jnp.sqrt((own + core) + (chip + both))


def gathered(blocks):
    me = lax.axis_index("shard")
    rows = blocks[0].shape[1]
    total = len(blocks) * rows
    out = jnp.zeros((1, 4 * total, blocks[0].shape[2]), blocks[0].dtype)
    chips = [swap(b, "shard", CHIP) for b in blocks]
    cores = [swap(b, "shard", CORE) for b in blocks]
    boths = [swap(b, "shard", CORE) for b in chips]
    for mask, pieces in ((0, blocks), (CORE, cores), (CHIP, chips), (CORE | CHIP, boths)):
        for k, piece in enumerate(pieces):
            out = lax.dynamic_update_slice(out, piece, (0, (me ^ mask) * total + k * rows, 0))
    return out


def doubled(x, axis, mask, dim):
    other = swap(x, axis, mask)
    low = (lax.axis_index(axis) & mask) == 0
    return jnp.concatenate([jnp.where(low, x, other), jnp.where(low, other, x)], axis=dim)


def per_device(w_gate, avg_gate, w_up, avg_up, mix_share, router_weight, router_gain):
    share = mix_share[:, None, None]
    fresh_gate = share * w_gate + (1.0 - share) * avg_gate
    fresh_up = share * w_up + (1.0 - share) * avg_up
    scale_gate = scales(fresh_gate)
    scale_up = scales(fresh_up)
    narrow_gate = (fresh_gate / scale_gate[:, None]).astype(jnp.bfloat16)
    narrow_up = (fresh_up / scale_up[:, None]).astype(jnp.bfloat16)
    serve_gate = gathered(jnp.split(narrow_gate, PIECES, axis=1))
    serve_up = gathered(jnp.split(narrow_up, PIECES, axis=1))

    part = (router_weight[:, 0] * router_gain).astype(jnp.bfloat16)
    router = doubled(part[None, None, :], "shard", CHIP, 1)
    for mask in (16, 32, 4, 8, 1, 2):
        router = doubled(router, "expert", mask, 0)
    router = doubled(router[:, :, None, :], "shard", CORE, 2)
    router = router.reshape(2, 2, 2, 2, 2, 2, -1)
    router = router.transpose(4, 5, 2, 3, 0, 1, 6).reshape(64, -1)
    return (serve_gate, serve_up, scale_gate, scale_up, router.T)


def solution(mesh):
    return jax.shard_map(
        per_device,
        mesh=mesh,
        in_specs=(
            P("expert", "shard", None),
            P("expert", "shard", None),
            P("expert", "shard", None),
            P("expert", "shard", None),
            P("expert"),
            P("shard", "expert"),
            P("shard"),
        ),
        out_specs=(
            P("expert", None, None),
            P("expert", None, None),
            P("expert", None),
            P("expert", None),
            P(),
        ),
        check_vma=False,
    )
```

```python
import functools

import jax
import jax.numpy as jnp
from jax import lax
from jax.experimental import pallas as pl
from jax.experimental.pallas import tpu as pltpu
from jax.sharding import PartitionSpec as P


CORE, CHIP = 1, 2
GATE = (64, 256, 192)
UP = (256, 128, 64, 64)
LOADS = 8
MIB = 1 << 20
VMEM = pl.BlockSpec(memory_space=pltpu.VMEM)
HBM = pl.BlockSpec(memory_space=pltpu.HBM)
SMEM = pl.BlockSpec(memory_space=pltpu.SMEM)


def swap(x, axis, mask):
    n = lax.axis_size(axis)
    return lax.ppermute(x, axis, [(i, i ^ mask) for i in range(n)])


def call(body, out, ins, mib, flops, **kw):
    return pl.pallas_call(
        body,
        out_shape=out,
        compiler_params=pltpu.CompilerParams(vmem_limit_bytes=mib * MIB),
        cost_estimate=pl.CostEstimate(flops=flops, bytes_accessed=4 * MIB, transcendentals=0),
        in_specs=ins,
        **kw,
    )


def mean_body(share_ref, w_ref, avg_ref, fresh_ref, sums_ref, w_buf, avg_buf, sem):
    rows = w_buf.shape[0]
    step = rows // LOADS

    def copies(k):
        at = pl.ds(k * step, step)
        return (
            pltpu.make_async_copy(w_ref.at[0, at], w_buf.at[at], sem.at[0, k]),
            pltpu.make_async_copy(avg_ref.at[0, at], avg_buf.at[at], sem.at[1, k]),
        )

    for k in range(LOADS):
        for c in copies(k):
            c.start()
    share = share_ref[0]
    rest = 1.0 - share
    total = jnp.zeros((8, w_buf.shape[1]), jnp.float32)
    for k in range(LOADS):
        for c in copies(k):
            c.wait()

        def tile(i, total):
            at = pl.ds(pl.multiple_of(k * step + i * 8, 8), 8)
            fresh = share * w_buf[at] + rest * avg_buf[at]
            fresh_ref[at] = fresh
            return total + fresh * fresh

        total = lax.fori_loop(0, step // 8, tile, total, unroll=True)
    sums_ref[...] = jnp.sum(total, axis=0, keepdims=True)


def mean_of(share, w, avg, mib):
    _, rows, columns = w.shape
    return call(
        mean_body,
        (pltpu.VMEM((rows, columns), jnp.float32), pltpu.VMEM((1, columns), jnp.float32)),
        [SMEM, HBM, HBM],
        mib,
        4 << 20,
        out_specs=(VMEM, VMEM),
        scratch_shapes=[
            pltpu.VMEM((rows, columns), jnp.float32),
            pltpu.VMEM((rows, columns), jnp.float32),
            pltpu.SemaphoreType.DMA((2, LOADS)),
        ],
    )(share, w, avg)


def narrow_body(first, blocks, scaled, fresh_ref, pair_ref, other_ref, *outs):
    columns = fresh_ref.shape[1]
    scale = jnp.sqrt(pair_ref[:, :columns] + other_ref[:, :columns])
    if scaled:
        outs[-1][...] = scale
    inverse = 1.0 / scale
    at = first
    for rows, out in zip(blocks, outs):
        for i in range(rows // 16):
            out[0, pl.ds(i * 16, 16)] = (fresh_ref[pl.ds(at + i * 16, 16)] * inverse).astype(out.dtype)
        at += rows


def narrow(fresh, totals, first, blocks, scaled):
    columns = fresh.shape[1]
    outs = [pltpu.VMEM((1, rows, columns), jnp.bfloat16) for rows in blocks]
    if scaled:
        outs.append(jax.ShapeDtypeStruct((1, columns), jnp.float32))
    return call(
        functools.partial(narrow_body, first, blocks, scaled),
        tuple(outs),
        [VMEM, VMEM, VMEM],
        2,
        2 << 20,
        out_specs=(VMEM,) * len(outs),
    )(fresh, *totals)


def place_body(places, *refs):
    out, sem = refs[-2], refs[-1]
    me = lax.axis_index("shard")
    copies = []
    for k, (mask, at, rows, shard_rows) in enumerate(places):
        start = pl.multiple_of((me ^ mask) * shard_rows + at, 16)
        copies.append(pltpu.make_async_copy(refs[k].at[0], out.at[0, pl.ds(start, rows)], sem.at[k]))
    for c in copies:
        c.start()
    for c in copies:
        c.wait()


def place(pieces, shape, into=None):
    blocks = [p[0] for p in pieces]
    places = tuple((m, at, b.shape[1], total) for b, m, at, total in pieces)
    n = len(blocks)
    again = into is not None
    return call(
        functools.partial(place_body, places),
        jax.ShapeDtypeStruct(shape, blocks[0].dtype),
        [VMEM] * n + [HBM] * again,
        6,
        1 << 20,
        out_specs=HBM,
        scratch_shapes=[pltpu.SemaphoreType.DMA((n,))],
        **({"input_output_aliases": {n: 0}} if again else {}),
    )(*blocks, *([into] if again else []))


def starts(blocks):
    at, out = 0, []
    for rows in blocks:
        out.append(at)
        at += rows
    return out


def from_all(own):
    chips = [swap(b, "shard", CHIP) for b in own]
    cores = [swap(b, "shard", CORE) for b in own]
    boths = [swap(b, "shard", CORE) for b in chips]
    return {0: own, CORE: cores, CHIP: chips, CORE | CHIP: boths}


BITS = (("shard", CHIP), ("expert", 16), ("expert", 32), ("expert", 1), ("expert", 2), ("expert", 4), ("expert", 8))


def lows_body(*outs):
    for (axis, mask), out in zip(BITS, outs):
        low = jnp.where((lax.axis_index(axis) & mask) == 0, 1.0, 0.0)
        out[...] = jnp.full(out.shape, low, jnp.float32)


def lows_of(rows):
    outs = call(
        lows_body,
        tuple(jax.ShapeDtypeStruct((1, rows), jnp.float32) for _ in BITS),
        [],
        1,
        1 << 10,
        out_specs=(VMEM,) * len(BITS),
    )()
    return dict(zip(BITS, outs))


def in_order(low, own, other, dim):
    low = low.reshape((1,) * (own.ndim - 2) + low.shape) > 0.5
    return jnp.concatenate([jnp.where(low, own, other), jnp.where(low, other, own)], axis=dim)


def router_body(own_ref, other_ref, out_ref):
    z, chips, plane, rows = own_ref.shape
    first = (lax.axis_index("shard") & CORE) == 0
    for k in range(z):
        for chip in range(chips):
            own, other = own_ref[k, chip], other_ref[k, chip]
            for core in range(2):
                at = (chip * 2 + core) * rows
                value = jnp.where(first, own, other) if core == 0 else jnp.where(first, other, own)
                out_ref[pl.ds(k * plane, plane), pl.ds(at, rows)] = value


def router_of(lows, own, other):
    x = in_order(lows["shard", CHIP], own[None, None], other[None, None], 1)
    z1, z2, z3 = (swap(x, "expert", 16 * k) for k in (1, 2, 3))
    bit = lows["expert", 16]
    x = in_order(lows["expert", 32], in_order(bit, x, z1, 0), in_order(bit, z2, z3, 0), 0)
    for mask in (1, 2, 4, 8):
        x = in_order(lows["expert", mask], x, swap(x, "expert", mask), 2)
    other = swap(x, "shard", CORE)
    z, chips, plane, rows = x.shape
    return call(
        router_body,
        jax.ShapeDtypeStruct((z * plane, chips * 2 * rows), x.dtype),
        [VMEM, VMEM],
        2,
        1 << 20,
        out_specs=VMEM,
    )(x, other).T


def per_device(w_gate, avg_gate, w_up, avg_up, mix_share, router_weight, router_gain):
    rows, columns = w_gate.shape[1:]
    shape = (1, lax.axis_size("shard") * rows, columns)
    part = (router_weight.T * router_gain[None]).astype(jnp.bfloat16)
    lows = lows_of(rows)

    fresh_gate, sums_gate = mean_of(mix_share, w_gate, avg_gate, 60)
    pair = sums_gate + swap(sums_gate, "shard", CORE)
    pair = jnp.concatenate([pair, part.astype(jnp.float32)], axis=1)
    totals_gate = pair, swap(pair, "shard", CHIP)
    (gate_0,) = narrow(fresh_gate, totals_gate, 0, GATE[:1], False)
    *gate_rest, scale_gate = narrow(fresh_gate, totals_gate, GATE[0], GATE[1:], True)
    gate = from_all([gate_0, *gate_rest])

    fresh_up, sums_up = mean_of(mix_share, w_up, avg_up, 56)
    pair = sums_up + swap(sums_up, "shard", CORE)
    totals_up = pair, swap(pair, "shard", CHIP)
    *own_up, scale_up = narrow(fresh_up, totals_up, 0, UP, True)
    up = from_all(own_up)

    gate_at, up_at = starts(GATE), starts(UP)
    serve_gate = place(
        [(b, m, at, rows) for m, bs in gate.items() for b, at in zip(bs, gate_at)], shape
    )
    early, late = [], []
    for m, bs in up.items():
        for k, (b, at) in enumerate(zip(bs, up_at)):
            (late if m & CHIP and k >= 2 else early).append((b, m, at, rows))
    serve_up = place(late, shape, place(early, shape))

    other = totals_gate[1][:, columns:].astype(jnp.bfloat16)
    serve_router = router_of(lows, part, other)
    return (serve_gate, serve_up, scale_gate, scale_up, serve_router)


def solution(mesh):
    return jax.shard_map(
        per_device,
        mesh=mesh,
        in_specs=(
            P("expert", "shard", None),
            P("expert", "shard", None),
            P("expert", "shard", None),
            P("expert", "shard", None),
            P("expert"),
            P("shard", "expert"),
            P("shard"),
        ),
        out_specs=(
            P("expert", None, None),
            P("expert", None, None),
            P("expert", None),
            P("expert", None),
            P(),
        ),
        check_vma=False,
    )
```

```python
import functools

import jax
import jax.numpy as jnp
from jax import lax
from jax.experimental import pallas as pl
from jax.experimental.pallas import tpu as pltpu
from jax.sharding import PartitionSpec as P


CORE, CHIP = 1, 2
GATE = (256, 256)
UP = (256, 128, 64, 64)
LOADS = 8
MIB = 1 << 20
VMEM = pl.BlockSpec(memory_space=pltpu.VMEM)
SMEM = pl.BlockSpec(memory_space=pltpu.SMEM)
HBM = pl.BlockSpec(memory_space=pltpu.HBM)


def swap(x, axis, mask):
    n = lax.axis_size(axis)
    return lax.ppermute(x, axis, [(i, i ^ mask) for i in range(n)])


def call(body, out, ins, mib, flops, **kw):
    return pl.pallas_call(
        body,
        out_shape=out,
        compiler_params=pltpu.CompilerParams(vmem_limit_bytes=mib * MIB),
        cost_estimate=pl.CostEstimate(flops=flops, bytes_accessed=4 * MIB, transcendentals=0),
        in_specs=ins,
        **kw,
    )


def mean_body(share_ref, w_ref, avg_ref, fresh_ref, sums_ref, w_buf, avg_buf, sem):
    rows = w_buf.shape[0]
    step = rows // LOADS

    def copies(k):
        at = pl.ds(k * step, step)
        return (
            pltpu.make_async_copy(w_ref.at[0, at], w_buf.at[at], sem.at[0, k]),
            pltpu.make_async_copy(avg_ref.at[0, at], avg_buf.at[at], sem.at[1, k]),
        )

    for k in range(LOADS):
        for c in copies(k):
            c.start()
    share = share_ref[0]
    rest = 1.0 - share
    total = jnp.zeros((8, w_buf.shape[1]), jnp.float32)
    for k in range(LOADS):
        for c in copies(k):
            c.wait()

        def tile(i, total):
            at = pl.ds(pl.multiple_of(k * step + i * 8, 8), 8)
            fresh = share * w_buf[at] + rest * avg_buf[at]
            fresh_ref[at] = fresh
            return total + fresh * fresh

        total = lax.fori_loop(0, step // 8, tile, total, unroll=True)
    sums_ref[...] = jnp.sum(total, axis=0, keepdims=True)


def mean_of(share, w, avg, mib):
    _, rows, columns = w.shape
    return call(
        mean_body,
        (pltpu.VMEM((rows, columns), jnp.float32), pltpu.VMEM((1, columns), jnp.float32)),
        [SMEM, HBM, HBM],
        mib,
        4 << 20,
        out_specs=(VMEM, VMEM),
        scratch_shapes=[
            pltpu.VMEM((rows, columns), jnp.float32),
            pltpu.VMEM((rows, columns), jnp.float32),
            pltpu.SemaphoreType.DMA((2, LOADS)),
        ],
    )(share, w, avg)


def narrow_body(first, blocks, scaled, fresh_ref, pair_ref, other_ref, *outs):
    columns = fresh_ref.shape[1]
    scale = jnp.sqrt(pair_ref[:, :columns] + other_ref[:, :columns])
    if scaled:
        outs[-1][...] = scale
    inverse = 1.0 / scale
    at = first
    for rows, out in zip(blocks, outs):
        for i in range(rows // 16):
            out[0, pl.ds(i * 16, 16)] = (fresh_ref[pl.ds(at + i * 16, 16)] * inverse).astype(out.dtype)
        at += rows


def narrow(fresh, totals, first, blocks, scaled):
    columns = fresh.shape[1]
    outs = [pltpu.VMEM((1, rows, columns), jnp.bfloat16) for rows in blocks]
    if scaled:
        outs.append(jax.ShapeDtypeStruct((1, columns), jnp.float32))
    return call(
        functools.partial(narrow_body, first, blocks, scaled),
        tuple(outs),
        [VMEM, VMEM, VMEM],
        2,
        2 << 20,
        out_specs=(VMEM,) * len(outs),
    )(fresh, *totals)


def place_body(places, *refs):
    out, sem = refs[-2], refs[-1]
    me = lax.axis_index("shard")
    copies = []
    for k, (mask, at, rows, shard_rows) in enumerate(places):
        start = pl.multiple_of((me ^ mask) * shard_rows + at, 16)
        copies.append(pltpu.make_async_copy(refs[k].at[0], out.at[0, pl.ds(start, rows)], sem.at[k]))
    for c in copies:
        c.start()
    for c in copies:
        c.wait()


def place(pieces, shape, into=None):
    blocks = [p[0] for p in pieces]
    places = tuple((m, at, b.shape[1], total) for b, m, at, total in pieces)
    n = len(blocks)
    again = into is not None
    return call(
        functools.partial(place_body, places),
        jax.ShapeDtypeStruct(shape, blocks[0].dtype),
        [VMEM] * n + [HBM] * again,
        6,
        1 << 20,
        out_specs=HBM,
        scratch_shapes=[pltpu.SemaphoreType.DMA((n,))],
        **({"input_output_aliases": {n: 0}} if again else {}),
    )(*blocks, *([into] if again else []))


def starts(blocks):
    at, out = 0, []
    for rows in blocks:
        out.append(at)
        at += rows
    return out


def from_all(own):
    chips = [swap(b, "shard", CHIP) for b in own]
    cores = [swap(b, "shard", CORE) for b in own]
    boths = [swap(b, "shard", CORE) for b in chips]
    return {0: own, CORE: cores, CHIP: chips, CORE | CHIP: boths}


BITS = (("shard", CHIP), ("expert", 1), ("expert", 2), ("expert", 4), ("expert", 8))


def lows_body(*outs):
    for (axis, mask), out in zip(BITS, outs):
        low = jnp.where((lax.axis_index(axis) & mask) == 0, 1.0, 0.0)
        out[...] = jnp.full(out.shape, low, jnp.float32)


def lows_of(rows):
    outs = call(
        lows_body,
        tuple(jax.ShapeDtypeStruct((1, rows), jnp.float32) for _ in BITS),
        [],
        1,
        1 << 10,
        out_specs=(VMEM,) * len(BITS),
    )()
    return dict(zip(BITS, outs))


def in_order(low, own, other, dim):
    low = low.reshape((1,) * (own.ndim - 2) + low.shape) > 0.5
    return jnp.concatenate([jnp.where(low, own, other), jnp.where(low, other, own)], axis=dim)


def router_body(own_ref, other_ref, out_ref):
    z, chips, plane, rows = own_ref.shape
    first = (lax.axis_index("shard") & CORE) == 0
    for k in range(z):
        for chip in range(chips):
            own, other = own_ref[k, chip], other_ref[k, chip]
            for core in range(2):
                at = (chip * 2 + core) * rows
                value = jnp.where(first, own, other) if core == 0 else jnp.where(first, other, own)
                out_ref[pl.ds(k * plane, plane), pl.ds(at, rows)] = value


def planes_body(*refs):
    z = lax.axis_index("expert") // 16
    for k, ref in enumerate(refs[:-1]):
        refs[-1][z ^ k] = ref[0]


def router_of(lows, own, other):
    x = in_order(lows["shard", CHIP], own[None, None], other[None, None], 1)
    pieces = (x, *(swap(x, "expert", 16 * k) for k in (1, 2, 3)))
    x = call(
        planes_body,
        jax.ShapeDtypeStruct((4, *x.shape[1:]), x.dtype),
        [VMEM] * 4,
        1,
        1 << 10,
        out_specs=VMEM,
    )(*pieces)
    for unit in (1, 4):
        a, b, c = (swap(x, "expert", unit * k) for k in (1, 2, 3))
        low = lows["expert", unit]
        x = in_order(lows["expert", 2 * unit], in_order(low, x, a, 2), in_order(low, b, c, 2), 2)
    other = swap(x, "shard", CORE)
    z, chips, plane, rows = x.shape
    return call(
        router_body,
        jax.ShapeDtypeStruct((z * plane, chips * 2 * rows), x.dtype),
        [VMEM, VMEM],
        2,
        1 << 20,
        out_specs=VMEM,
    )(x, other).T


def per_device(w_gate, avg_gate, w_up, avg_up, mix_share, router_weight, router_gain):
    rows, columns = w_gate.shape[1:]
    shape = (1, lax.axis_size("shard") * rows, columns)
    part = (router_weight.T * router_gain[None]).astype(jnp.bfloat16)
    lows = lows_of(rows)

    fresh_gate, sums_gate = mean_of(mix_share, w_gate, avg_gate, 60)
    pair = sums_gate + swap(sums_gate, "shard", CORE)
    pair = jnp.concatenate([pair, part.astype(jnp.float32)], axis=1)
    totals_gate = pair, swap(pair, "shard", CHIP)
    (gate_0,) = narrow(fresh_gate, totals_gate, 0, GATE[:1], False)
    *gate_rest, scale_gate = narrow(fresh_gate, totals_gate, GATE[0], GATE[1:], True)
    gate = from_all([gate_0, *gate_rest])

    fresh_up, sums_up = mean_of(mix_share, w_up, avg_up, 56)
    pair = sums_up + swap(sums_up, "shard", CORE)
    totals_up = pair, swap(pair, "shard", CHIP)
    *own_up, scale_up = narrow(fresh_up, totals_up, 0, UP, True)
    up = from_all(own_up)

    gate_at, up_at = starts(GATE), starts(UP)
    serve_gate = place(
        [(b, m, at, rows) for m, bs in gate.items() for b, at in zip(bs, gate_at)], shape
    )
    early, late = [], []
    for m, bs in up.items():
        for k, (b, at) in enumerate(zip(bs, up_at)):
            (late if m & CHIP and k >= 2 else early).append((b, m, at, rows))
    serve_up = place(late, shape, place(early, shape))

    other = totals_gate[1][:, columns:].astype(jnp.bfloat16)
    serve_router = router_of(lows, part, other)
    return (serve_gate, serve_up, scale_gate, scale_up, serve_router)


def solution(mesh):
    return jax.shard_map(
        per_device,
        mesh=mesh,
        in_specs=(
            P("expert", "shard", None),
            P("expert", "shard", None),
            P("expert", "shard", None),
            P("expert", "shard", None),
            P("expert"),
            P("shard", "expert"),
            P("shard"),
        ),
        out_specs=(
            P("expert", None, None),
            P("expert", None, None),
            P("expert", None),
            P("expert", None),
            P(),
        ),
        check_vma=False,
    )
```

```python
import functools

import jax
import jax.numpy as jnp
from jax import lax
from jax.experimental import pallas as pl
from jax.experimental.pallas import tpu as pltpu
from jax.sharding import PartitionSpec as P


CORE, CHIP = 1, 2
GATE = (64, 192, 256)
UP = (256, 128, 64, 64)
LOADS = 8
MIB = 1 << 20
VMEM = pl.BlockSpec(memory_space=pltpu.VMEM)
SMEM = pl.BlockSpec(memory_space=pltpu.SMEM)
HBM = pl.BlockSpec(memory_space=pltpu.HBM)


def swap(x, axis, mask):
    n = lax.axis_size(axis)
    return lax.ppermute(x, axis, [(i, i ^ mask) for i in range(n)])


def call(body, out, ins, mib, flops, **kw):
    return pl.pallas_call(
        body,
        out_shape=out,
        compiler_params=pltpu.CompilerParams(vmem_limit_bytes=mib * MIB),
        cost_estimate=pl.CostEstimate(flops=flops, bytes_accessed=4 * MIB, transcendentals=0),
        in_specs=ins,
        **kw,
    )


def mean_body(share_ref, w_ref, avg_ref, fresh_ref, sums_ref, w_buf, avg_buf, sem):
    rows = w_buf.shape[0]
    step = rows // LOADS

    def copies(k):
        at = pl.ds(k * step, step)
        return (
            pltpu.make_async_copy(w_ref.at[0, at], w_buf.at[at], sem.at[0, k]),
            pltpu.make_async_copy(avg_ref.at[0, at], avg_buf.at[at], sem.at[1, k]),
        )

    for k in range(LOADS):
        for c in copies(k):
            c.start()
    share = share_ref[0]
    rest = 1.0 - share
    total = jnp.zeros((8, w_buf.shape[1]), jnp.float32)
    for k in range(LOADS):
        for c in copies(k):
            c.wait()

        def tile(i, total):
            at = pl.ds(pl.multiple_of(k * step + i * 8, 8), 8)
            fresh = share * w_buf[at] + rest * avg_buf[at]
            fresh_ref[at] = fresh
            return total + fresh * fresh

        total = lax.fori_loop(0, step // 8, tile, total, unroll=True)
    sums_ref[...] = jnp.sum(total, axis=0, keepdims=True)


def mean_of(share, w, avg, mib):
    _, rows, columns = w.shape
    return call(
        mean_body,
        (pltpu.VMEM((rows, columns), jnp.float32), pltpu.VMEM((1, columns), jnp.float32)),
        [SMEM, HBM, HBM],
        mib,
        4 << 20,
        out_specs=(VMEM, VMEM),
        scratch_shapes=[
            pltpu.VMEM((rows, columns), jnp.float32),
            pltpu.VMEM((rows, columns), jnp.float32),
            pltpu.SemaphoreType.DMA((2, LOADS)),
        ],
    )(share, w, avg)


def narrow_body(first, blocks, whole, fresh_ref, pair_ref, other_ref, *outs):
    columns = fresh_ref.shape[1]
    inverse = 1.0 / jnp.sqrt(pair_ref[:, :columns] + other_ref[:, :columns])

    def rows_of(at):
        return (fresh_ref[pl.ds(at, 16)] * inverse).astype(jnp.bfloat16)

    if whole:
        for at in range(0, first, 16):
            outs[-1][0, pl.ds(at, 16)] = rows_of(at)
    at = first
    for rows, out in zip(blocks, outs):
        for i in range(0, rows, 16):
            value = rows_of(at + i)
            out[0, pl.ds(i, 16)] = value
            if whole:
                outs[-1][0, pl.ds(at + i, 16)] = value
        at += rows


def narrow(fresh, totals, first, blocks, whole):
    rows, columns = fresh.shape
    sizes = [*blocks, rows] if whole else blocks
    outs = tuple(pltpu.VMEM((1, n, columns), jnp.bfloat16) for n in sizes)
    return call(
        functools.partial(narrow_body, first, blocks, whole),
        outs,
        [VMEM, VMEM, VMEM],
        2,
        2 << 20,
        out_specs=(VMEM,) * len(outs),
    )(fresh, *totals)


def place_body(places, *refs):
    out, sem = refs[-2], refs[-1]
    me = lax.axis_index("shard")
    copies = []
    for k, (mask, at, rows, shard_rows) in enumerate(places):
        start = pl.multiple_of((me ^ mask) * shard_rows + at, 16)
        copies.append(pltpu.make_async_copy(refs[k].at[0], out.at[0, pl.ds(start, rows)], sem.at[k]))
    for c in copies:
        c.start()
    for c in copies:
        c.wait()


def place(pieces, shard_rows, shape, into=None):
    blocks = [p[0] for p in pieces]
    places = tuple((m, at, b.shape[1], shard_rows) for b, m, at in pieces)
    n = len(blocks)
    again = into is not None
    return call(
        functools.partial(place_body, places),
        jax.ShapeDtypeStruct(shape, blocks[0].dtype),
        [VMEM] * n + [HBM] * again,
        6,
        1 << 20,
        out_specs=HBM,
        scratch_shapes=[pltpu.SemaphoreType.DMA((n,))],
        **({"input_output_aliases": {n: 0}} if again else {}),
    )(*blocks, *([into] if again else []))


def starts(blocks):
    at, out = 0, []
    for rows in blocks:
        out.append(at)
        at += rows
    return out


def from_all(blocks, whole):
    chips = [swap(b, "shard", CHIP) for b in blocks]
    boths = [swap(b, "shard", CORE) for b in chips]
    at = starts([b.shape[1] for b in blocks])
    near = [(whole, 0, 0), (swap(whole, "shard", CORE), CORE, 0)]
    far = [[(c, CHIP, n), (b, CORE | CHIP, n)] for c, b, n in zip(chips, boths, at)]
    return near, far


BITS = (("shard", CHIP), ("expert", 1), ("expert", 2), ("expert", 4), ("expert", 8))


def lows_body(*outs):
    for (axis, mask), out in zip(BITS, outs):
        low = jnp.where((lax.axis_index(axis) & mask) == 0, 1.0, 0.0)
        out[...] = jnp.full(out.shape, low, jnp.float32)


def lows_of(rows):
    outs = call(
        lows_body,
        tuple(jax.ShapeDtypeStruct((1, rows), jnp.float32) for _ in BITS),
        [],
        1,
        1 << 10,
        out_specs=(VMEM,) * len(BITS),
    )()
    return dict(zip(BITS, outs))


def in_order(low, own, other, dim):
    low = low.reshape((1,) * (own.ndim - 2) + low.shape) > 0.5
    return jnp.concatenate([jnp.where(low, own, other), jnp.where(low, other, own)], axis=dim)


def router_body(own_ref, other_ref, out_ref):
    z, chips, plane, rows = own_ref.shape
    first = (lax.axis_index("shard") & CORE) == 0
    for k in range(z):
        for chip in range(chips):
            own, other = own_ref[k, chip], other_ref[k, chip]
            for core in range(2):
                at = (chip * 2 + core) * rows
                value = jnp.where(first, own, other) if core == 0 else jnp.where(first, other, own)
                out_ref[pl.ds(k * plane, plane), pl.ds(at, rows)] = value


def turned(x):
    experts, shards = lax.axis_size("expert"), lax.axis_size("shard")
    pairs = []
    for e in range(experts):
        for s in range(shards):
            to = (e + (16 if s & CHIP else -16)) % experts
            pairs.append((e * shards + s, to * shards + s))
    return lax.ppermute(x, ("expert", "shard"), pairs)


def planes_body(*refs):
    z = lax.axis_index("expert") // 16
    up = (lax.axis_index("shard") & CHIP) == 0
    for k, ref in enumerate(refs[:-1]):
        refs[-1][jnp.where(up, z + k, z + 4 - k) % 4] = ref[0]


def router_of(lows, own, other):
    pieces = [in_order(lows["shard", CHIP], own[None, None], other[None, None], 1)]
    for _ in range(3):
        pieces.append(turned(pieces[-1]))
    x = pieces[0]
    x = call(
        planes_body,
        jax.ShapeDtypeStruct((4, *x.shape[1:]), x.dtype),
        [VMEM] * 4,
        1,
        1 << 10,
        out_specs=VMEM,
    )(*pieces)
    for unit in (1, 4):
        a, b, c = (swap(x, "expert", unit * k) for k in (1, 2, 3))
        low = lows["expert", unit]
        x = in_order(lows["expert", 2 * unit], in_order(low, x, a, 2), in_order(low, b, c, 2), 2)
    other = swap(x, "shard", CORE)
    z, chips, plane, rows = x.shape
    return call(
        router_body,
        jax.ShapeDtypeStruct((z * plane, chips * 2 * rows), x.dtype),
        [VMEM, VMEM],
        2,
        1 << 20,
        out_specs=VMEM,
    )(x, other).T


def scale_of(totals, columns):
    pair, other = totals
    return jnp.sqrt(pair[:, :columns] + other[:, :columns])


def per_device(w_gate, avg_gate, w_up, avg_up, mix_share, router_weight, router_gain):
    rows, columns = w_gate.shape[1:]
    shape = (1, lax.axis_size("shard") * rows, columns)
    part = (router_weight.T * router_gain[None]).astype(jnp.bfloat16)
    lows = lows_of(rows)

    fresh_gate, sums_gate = mean_of(mix_share, w_gate, avg_gate, 60)
    pair = sums_gate + swap(sums_gate, "shard", CORE)
    pair = jnp.concatenate([pair, part.astype(jnp.float32)], axis=1)
    totals_gate = pair, swap(pair, "shard", CHIP)
    scale_gate = scale_of(totals_gate, columns)
    gate = narrow(fresh_gate, totals_gate, 0, GATE[:1], False)
    *rest, whole = narrow(fresh_gate, totals_gate, GATE[0], GATE[1:], True)
    near, far = from_all([*gate, *rest], whole)
    serve_gate = place(sum(far, near), rows, shape)

    fresh_up, sums_up = mean_of(mix_share, w_up, avg_up, 56)
    pair = sums_up + swap(sums_up, "shard", CORE)
    totals_up = pair, swap(pair, "shard", CHIP)
    scale_up = scale_of(totals_up, columns)
    *up, whole = narrow(fresh_up, totals_up, 0, UP, True)
    near, far = from_all(up, whole)
    serve_up = place(sum(far[:2], near), rows, shape)
    serve_up = place(sum(far[2:], []), rows, shape, serve_up)

    other = totals_gate[1][:, columns:].astype(jnp.bfloat16)
    serve_router = router_of(lows, part, other)
    return (serve_gate, serve_up, scale_gate, scale_up, serve_router)


def solution(mesh):
    return jax.shard_map(
        per_device,
        mesh=mesh,
        in_specs=(
            P("expert", "shard", None),
            P("expert", "shard", None),
            P("expert", "shard", None),
            P("expert", "shard", None),
            P("expert"),
            P("shard", "expert"),
            P("shard"),
        ),
        out_specs=(
            P("expert", None, None),
            P("expert", None, None),
            P("expert", None),
            P("expert", None),
            P(),
        ),
        check_vma=False,
    )
```

```python
import functools

import jax
import jax.numpy as jnp
from jax import lax
from jax.experimental import pallas as pl
from jax.experimental.pallas import tpu as pltpu
from jax.sharding import PartitionSpec as P


CORE, CHIP = 1, 2
GATE = (64, 192, 256)
UP = (256, 128, 64, 64)
LOADS = 8
MIB = 1 << 20
VMEM = pl.BlockSpec(memory_space=pltpu.VMEM)
SMEM = pl.BlockSpec(memory_space=pltpu.SMEM)
HBM = pl.BlockSpec(memory_space=pltpu.HBM)


def swap(x, axis, mask):
    n = lax.axis_size(axis)
    return lax.ppermute(x, axis, [(i, i ^ mask) for i in range(n)])


def call(body, out, ins, mib, flops, **kw):
    return pl.pallas_call(
        body,
        out_shape=out,
        compiler_params=pltpu.CompilerParams(vmem_limit_bytes=mib * MIB),
        cost_estimate=pl.CostEstimate(flops=flops, bytes_accessed=4 * MIB, transcendentals=0),
        in_specs=ins,
        **kw,
    )


def mean_body(extras, share_ref, w_ref, avg_ref, *refs):
    extra_refs, (fresh_ref, sums_ref, w_buf, avg_buf, extra_buf, sem, extra_sem) = refs[:extras], refs[extras:]
    rows, columns = w_buf.shape
    step = rows // LOADS

    def copies(k):
        at = pl.ds(k * step, step)
        return (
            pltpu.make_async_copy(w_ref.at[0, at], w_buf.at[at], sem.at[0, k]),
            pltpu.make_async_copy(avg_ref.at[0, at], avg_buf.at[at], sem.at[1, k]),
        )

    extra = [pltpu.make_async_copy(r, extra_buf.at[k], extra_sem.at[k]) for k, r in enumerate(extra_refs)]
    for k in range(LOADS):
        for c in copies(k):
            c.start()
        if k == 0:
            for c in extra:
                c.start()
    share = share_ref[0]
    rest = 1.0 - share
    total = jnp.zeros((8, columns), jnp.float32)
    for k in range(LOADS):
        for c in copies(k):
            c.wait()

        def tile(i, total):
            at = pl.ds(pl.multiple_of(k * step + i * 8, 8), 8)
            fresh = share * w_buf[at] + rest * avg_buf[at]
            fresh_ref[at] = fresh
            return total + fresh * fresh

        total = lax.fori_loop(0, step // 8, tile, total, unroll=True)
    sums_ref[:, pl.ds(0, columns)] = jnp.sum(total, axis=0, keepdims=True)
    if extras:
        for c in extra:
            c.wait()
        product = (extra_buf[0] * extra_buf[1]).astype(jnp.bfloat16).astype(jnp.float32)
        sums_ref[:, pl.ds(columns, rows)] = product


def mean_of(share, w, avg, mib, *extra):
    _, rows, columns = w.shape
    n = len(extra)
    return call(
        functools.partial(mean_body, n),
        (
            pltpu.VMEM((rows, columns), jnp.float32),
            pltpu.VMEM((1, columns + (rows if n else 0)), jnp.float32),
        ),
        [SMEM] + [HBM] * (2 + n),
        mib,
        4 << 20,
        out_specs=(VMEM, VMEM),
        scratch_shapes=[
            pltpu.VMEM((rows, columns), jnp.float32),
            pltpu.VMEM((rows, columns), jnp.float32),
            pltpu.VMEM((2, 1, rows), jnp.float32),
            pltpu.SemaphoreType.DMA((2, LOADS)),
            pltpu.SemaphoreType.DMA((2,)),
        ],
    )(share, w, avg, *extra)


def narrow_body(first, blocks, whole, scales, fresh_ref, *refs):
    columns = fresh_ref.shape[1]
    totals, outs = refs[: 2 * max(scales, 1)], refs[2 * max(scales, 1) :]
    scale = [jnp.sqrt(a[:, :columns] + b[:, :columns]) for a, b in zip(totals[::2], totals[1::2])]
    inverse = 1.0 / scale[0]
    if scales:
        for value, out in zip(scale, outs[-scales:]):
            out[...] = value
        outs = outs[:-scales]

    def rows_of(at):
        return (fresh_ref[pl.ds(at, 16)] * inverse).astype(jnp.bfloat16)

    if whole:
        for at in range(0, first, 16):
            outs[-1][0, pl.ds(at, 16)] = rows_of(at)
    at = first
    for rows, out in zip(blocks, outs):
        for i in range(0, rows, 16):
            value = rows_of(at + i)
            out[0, pl.ds(i, 16)] = value
            if whole:
                outs[-1][0, pl.ds(at + i, 16)] = value
        at += rows


def narrow(fresh, totals, first, blocks, whole, scales=0):
    rows, columns = fresh.shape
    sizes = [*blocks, rows] if whole else blocks
    outs = [pltpu.VMEM((1, n, columns), jnp.bfloat16) for n in sizes]
    outs += [jax.ShapeDtypeStruct((1, columns), jnp.float32)] * scales
    return call(
        functools.partial(narrow_body, first, blocks, whole, scales),
        tuple(outs),
        [VMEM] * (1 + len(totals)),
        2,
        2 << 20,
        out_specs=(VMEM,) * len(outs),
    )(fresh, *totals)


def place_body(places, *refs):
    out, sem = refs[-2], refs[-1]
    me = lax.axis_index("shard")
    copies = []
    for k, (mask, at, rows, shard_rows) in enumerate(places):
        start = pl.multiple_of((me ^ mask) * shard_rows + at, 16)
        copies.append(pltpu.make_async_copy(refs[k].at[0], out.at[0, pl.ds(start, rows)], sem.at[k]))
    for c in copies:
        c.start()
    for c in copies:
        c.wait()


def place(pieces, shard_rows, shape, into=None):
    blocks = [p[0] for p in pieces]
    places = tuple((m, at, b.shape[1], shard_rows) for b, m, at in pieces)
    n = len(blocks)
    again = into is not None
    return call(
        functools.partial(place_body, places),
        jax.ShapeDtypeStruct(shape, blocks[0].dtype),
        [VMEM] * n + [HBM] * again,
        6,
        1 << 20,
        out_specs=HBM,
        scratch_shapes=[pltpu.SemaphoreType.DMA((n,))],
        **({"input_output_aliases": {n: 0}} if again else {}),
    )(*blocks, *([into] if again else []))


def starts(blocks):
    at, out = 0, []
    for rows in blocks:
        out.append(at)
        at += rows
    return out


def from_all(blocks, whole):
    chips = [swap(b, "shard", CHIP) for b in blocks]
    boths = [swap(b, "shard", CORE) for b in chips]
    at = starts([b.shape[1] for b in blocks])
    near = [(whole, 0, 0), (swap(whole, "shard", CORE), CORE, 0)]
    far = [[(c, CHIP, n), (b, CORE | CHIP, n)] for c, b, n in zip(chips, boths, at)]
    return near, far


BITS = (("shard", CORE), ("shard", CHIP), ("expert", 1), ("expert", 2), ("expert", 4), ("expert", 8))


def lows_body(*outs):
    for (axis, mask), out in zip(BITS, outs):
        low = jnp.where((lax.axis_index(axis) & mask) == 0, 1.0, 0.0)
        out[...] = jnp.full(out.shape, low, jnp.float32)


def lows_of(rows, both):
    outs = call(
        lows_body,
        tuple(jax.ShapeDtypeStruct((1, rows if b == BITS[0] else both), jnp.float32) for b in BITS),
        [],
        1,
        1 << 10,
        out_specs=(VMEM,) * len(BITS),
    )()
    return dict(zip(BITS, outs))


def in_order(low, own, other, dim):
    low = low.reshape((1,) * (own.ndim - 2) + low.shape) > 0.5
    return jnp.concatenate([jnp.where(low, own, other), jnp.where(low, other, own)], axis=dim)


def router_body(own_ref, other_ref, out_ref):
    z, chips, plane, rows = own_ref.shape
    made = (lax.axis_index("shard") & CORE) == CORE
    for k in range(z):
        for chip in range(chips):
            value = jnp.where(made, own_ref[k, chip], other_ref[k, chip])
            out_ref[pl.ds(k * plane, plane), pl.ds(chip * rows, rows)] = value


def sent(x, to):
    experts, shards = lax.axis_size("expert"), lax.axis_size("shard")
    pairs = []
    for e in range(experts):
        for s in range(CORE, shards, 2):
            f, t = to(e, s)
            pairs.append((e * shards + s, f % experts * shards + t))
    return lax.ppermute(x, ("expert", "shard"), pairs)


def turned(x):
    return sent(x, lambda e, s: (e + (16 if s & CHIP else -16), s))


def planes_body(*refs):
    z = lax.axis_index("expert") // 16
    up = (lax.axis_index("shard") & CHIP) == 0
    for k, ref in enumerate(refs[:-1]):
        refs[-1][jnp.where(up, z + k, z + 4 - k) % 4] = ref[0]


def router_of(lows, own, other):
    pieces = [in_order(lows["shard", CHIP], own[None, None], other[None, None], 1)]
    for _ in range(3):
        pieces.append(turned(pieces[-1]))
    x = pieces[0]
    x = call(
        planes_body, jax.ShapeDtypeStruct((4, *x.shape[1:]), x.dtype), [VMEM] * 4, 1, 1 << 10, out_specs=VMEM
    )(*pieces)
    for unit in (1, 4):
        a, b, c = (sent(x, lambda e, s, k=k: (e ^ unit * k, s)) for k in (1, 2, 3))
        low = lows["expert", unit]
        x = in_order(lows["expert", 2 * unit], in_order(low, x, a, 2), in_order(low, b, c, 2), 2)
    other = sent(x, lambda e, s: (e, s ^ CORE))
    z, chips, plane, rows = x.shape
    return call(
        router_body, jax.ShapeDtypeStruct((z * plane, chips * rows), x.dtype), [VMEM, VMEM], 2, 1 << 20, out_specs=VMEM
    )(x, other).T


def per_device(w_gate, avg_gate, w_up, avg_up, mix_share, router_weight, router_gain):
    rows, columns = w_gate.shape[1:]
    shape = (1, lax.axis_size("shard") * rows, columns)
    lows = lows_of(rows, 2 * rows)

    fresh_gate, mine = mean_of(mix_share, w_gate, avg_gate, 60, router_weight.T, router_gain[None])
    near = swap(mine, "shard", CORE)
    router = in_order(lows["shard", CORE], mine[:, columns:], near[:, columns:], 1)
    pair = jnp.concatenate([mine[:, :columns] + near[:, :columns], router], axis=1)
    totals_gate = pair, swap(pair, "shard", CHIP)
    gate = narrow(fresh_gate, totals_gate, 0, GATE[:1], False)
    *rest, whole = narrow(fresh_gate, totals_gate, GATE[0], GATE[1:], True)
    near, far = from_all([*gate, *rest], whole)
    serve_gate = place(sum(far, near), rows, shape)

    fresh_up, sums_up = mean_of(mix_share, w_up, avg_up, 56)
    pair = sums_up + swap(sums_up, "shard", CORE)
    totals_up = pair, swap(pair, "shard", CHIP)
    *up, whole, scale_up, scale_gate = narrow(fresh_up, totals_up + totals_gate, 0, UP, True, scales=2)
    near, far = from_all(up, whole)
    serve_up = place(sum(far[:2], near), rows, shape)
    serve_up = place(sum(far[2:], []), rows, shape, serve_up)

    other = totals_gate[1][:, columns:].astype(jnp.bfloat16)
    serve_router = router_of(lows, router.astype(jnp.bfloat16), other)
    return (serve_gate, serve_up, scale_gate, scale_up, serve_router)


def solution(mesh):
    return jax.shard_map(
        per_device,
        mesh=mesh,
        in_specs=(
            P("expert", "shard", None),
            P("expert", "shard", None),
            P("expert", "shard", None),
            P("expert", "shard", None),
            P("expert"),
            P("shard", "expert"),
            P("shard"),
        ),
        out_specs=(
            P("expert", None, None),
            P("expert", None, None),
            P("expert", None),
            P("expert", None),
            P(),
        ),
        check_vma=False,
    )
```

```python
import functools

import jax
import jax.numpy as jnp
from jax import lax
from jax.experimental import pallas as pl
from jax.experimental.pallas import tpu as pltpu
from jax.sharding import PartitionSpec as P


CORE, CHIP = 1, 2
GATE = (64, 192, 256)
UP = (256, 128, 64, 64)
LOADS = 8
MIB = 1 << 20
VMEM = pl.BlockSpec(memory_space=pltpu.VMEM)
SMEM = pl.BlockSpec(memory_space=pltpu.SMEM)
HBM = pl.BlockSpec(memory_space=pltpu.HBM)


def swap(x, axis, mask):
    n = lax.axis_size(axis)
    return lax.ppermute(x, axis, [(i, i ^ mask) for i in range(n)])


def call(body, out, ins, mib, flops, **kw):
    return pl.pallas_call(
        body,
        out_shape=out,
        compiler_params=pltpu.CompilerParams(vmem_limit_bytes=mib * MIB),
        cost_estimate=pl.CostEstimate(flops=flops, bytes_accessed=4 * MIB, transcendentals=0),
        in_specs=ins,
        **kw,
    )


def mean_body(extras, share_ref, w_ref, avg_ref, *refs):
    extra_refs, (fresh_ref, sums_ref, w_buf, avg_buf, extra_buf, sem, extra_sem) = refs[:extras], refs[extras:]
    rows, columns = w_buf.shape
    step = rows // LOADS

    def copies(k):
        at = pl.ds(k * step, step)
        return (
            pltpu.make_async_copy(w_ref.at[0, at], w_buf.at[at], sem.at[0, k]),
            pltpu.make_async_copy(avg_ref.at[0, at], avg_buf.at[at], sem.at[1, k]),
        )

    extra = [pltpu.make_async_copy(r, extra_buf.at[k], extra_sem.at[k]) for k, r in enumerate(extra_refs)]
    for k in range(LOADS):
        for c in copies(k):
            c.start()
        if k == 0:
            for c in extra:
                c.start()
    share = share_ref[0]
    rest = 1.0 - share
    total = jnp.zeros((8, columns), jnp.float32)
    for k in range(LOADS):
        for c in copies(k):
            c.wait()

        def tile(i, total):
            at = pl.ds(pl.multiple_of(k * step + i * 8, 8), 8)
            fresh = share * w_buf[at] + rest * avg_buf[at]
            fresh_ref[at] = fresh
            return total + fresh * fresh

        total = lax.fori_loop(0, step // 8, tile, total, unroll=True)
    sums_ref[:, pl.ds(0, columns)] = jnp.sum(total, axis=0, keepdims=True)
    if extras:
        for c in extra:
            c.wait()
        product = (extra_buf[0] * extra_buf[1]).astype(jnp.bfloat16).astype(jnp.float32)
        sums_ref[:, pl.ds(columns, rows)] = product


def mean_of(share, w, avg, mib, *extra):
    _, rows, columns = w.shape
    n = len(extra)
    return call(
        functools.partial(mean_body, n),
        (
            pltpu.VMEM((rows, columns), jnp.float32),
            pltpu.VMEM((1, columns + (rows if n else 0)), jnp.float32),
        ),
        [SMEM] + [HBM] * (2 + n),
        mib,
        4 << 20,
        out_specs=(VMEM, VMEM),
        scratch_shapes=[
            pltpu.VMEM((rows, columns), jnp.float32),
            pltpu.VMEM((rows, columns), jnp.float32),
            pltpu.VMEM((2, 1, rows), jnp.float32),
            pltpu.SemaphoreType.DMA((2, LOADS)),
            pltpu.SemaphoreType.DMA((2,)),
        ],
    )(share, w, avg, *extra)


def narrow_body(first, blocks, whole, scales, fresh_ref, *refs):
    columns = fresh_ref.shape[1]
    totals, outs = refs[: 2 * max(scales, 1)], refs[2 * max(scales, 1) :]
    scale = [jnp.sqrt(a[:, :columns] + b[:, :columns]) for a, b in zip(totals[::2], totals[1::2])]
    inverse = 1.0 / scale[0]
    if scales:
        for value, out in zip(scale, outs[-scales:]):
            out[...] = value
        outs = outs[:-scales]

    def rows_of(at):
        return (fresh_ref[pl.ds(at, 16)] * inverse).astype(jnp.bfloat16)

    if whole:
        for at in range(0, first, 16):
            outs[-1][0, pl.ds(at, 16)] = rows_of(at)
    at = first
    for rows, out in zip(blocks, outs):
        for i in range(0, rows, 16):
            value = rows_of(at + i)
            out[0, pl.ds(i, 16)] = value
            if whole:
                outs[-1][0, pl.ds(at + i, 16)] = value
        at += rows


def narrow(fresh, totals, first, blocks, whole, scales=0):
    rows, columns = fresh.shape
    sizes = [*blocks, rows] if whole else blocks
    outs = [pltpu.VMEM((1, n, columns), jnp.bfloat16) for n in sizes]
    outs += [jax.ShapeDtypeStruct((1, columns), jnp.float32)] * scales
    return call(
        functools.partial(narrow_body, first, blocks, whole, scales),
        tuple(outs),
        [VMEM] * (1 + len(totals)),
        2,
        2 << 20,
        out_specs=(VMEM,) * len(outs),
    )(fresh, *totals)


def place_body(places, *refs):
    out, sem = refs[-2], refs[-1]
    me = lax.axis_index("shard")
    copies = []
    for k, (mask, at, rows, shard_rows) in enumerate(places):
        start = pl.multiple_of((me ^ mask) * shard_rows + at, 16)
        copies.append(pltpu.make_async_copy(refs[k].at[0], out.at[0, pl.ds(start, rows)], sem.at[k]))
    for c in copies:
        c.start()
    for c in copies:
        c.wait()


def place(pieces, shard_rows, shape, into=None):
    blocks = [p[0] for p in pieces]
    places = tuple((m, at, b.shape[1], shard_rows) for b, m, at in pieces)
    n = len(blocks)
    again = into is not None
    return call(
        functools.partial(place_body, places),
        jax.ShapeDtypeStruct(shape, blocks[0].dtype),
        [VMEM] * n + [HBM] * again,
        6,
        1 << 20,
        out_specs=HBM,
        scratch_shapes=[pltpu.SemaphoreType.DMA((n,))],
        **({"input_output_aliases": {n: 0}} if again else {}),
    )(*blocks, *([into] if again else []))


def starts(blocks):
    at, out = 0, []
    for rows in blocks:
        out.append(at)
        at += rows
    return out


def from_all(blocks, whole):
    chips = [swap(b, "shard", CHIP) for b in blocks]
    boths = [swap(b, "shard", CORE) for b in chips]
    at = starts([b.shape[1] for b in blocks])
    near = [(whole, 0, 0), (swap(whole, "shard", CORE), CORE, 0)]
    far = [[(c, CHIP, n), (b, CORE | CHIP, n)] for c, b, n in zip(chips, boths, at)]
    return near, far


BITS = (("shard", CORE), ("shard", CHIP), ("expert", 1), ("expert", 2), ("expert", 4), ("expert", 8))


def lows_body(*outs):
    for (axis, mask), out in zip(BITS, outs):
        low = jnp.where((lax.axis_index(axis) & mask) == 0, 1.0, 0.0)
        out[...] = jnp.full(out.shape, low, jnp.float32)


def lows_of(rows, both):
    outs = call(
        lows_body,
        tuple(jax.ShapeDtypeStruct((1, rows if b == BITS[0] else both), jnp.float32) for b in BITS),
        [],
        1,
        1 << 10,
        out_specs=(VMEM,) * len(BITS),
    )()
    return dict(zip(BITS, outs))


def in_order(low, own, other, dim):
    low = low.reshape((1,) * (own.ndim - 2) + low.shape) > 0.5
    return jnp.concatenate([jnp.where(low, own, other), jnp.where(low, other, own)], axis=dim)


def router_body(own_ref, other_ref, out_ref):
    z, chips, plane, rows = own_ref.shape
    made = (lax.axis_index("shard") & CORE) == CORE
    for k in range(z):
        for chip in range(chips):
            value = jnp.where(made, own_ref[k, chip], other_ref[k, chip])
            out_ref[pl.ds(k * plane, plane), pl.ds(chip * rows, rows)] = value


def sent(x, to):
    experts, shards = lax.axis_size("expert"), lax.axis_size("shard")
    pairs = []
    for e in range(experts):
        for s in range(shards):
            target = to(e, s) % experts if s & CORE else e
            pairs.append((e * shards + s, target * shards + s))
    return lax.ppermute(x, ("expert", "shard"), pairs)


def turned(x):
    return sent(x, lambda e, s: e + (16 if s & CHIP else -16))


def planes_body(*refs):
    z = lax.axis_index("expert") // 16
    up = (lax.axis_index("shard") & CHIP) == 0
    for k, ref in enumerate(refs[:-1]):
        refs[-1][jnp.where(up, z + k, z + 4 - k) % 4] = ref[0]


def router_of(lows, own, other):
    pieces = [in_order(lows["shard", CHIP], own[None, None], other[None, None], 1)]
    for _ in range(3):
        pieces.append(turned(pieces[-1]))
    x = pieces[0]
    x = call(
        planes_body, jax.ShapeDtypeStruct((4, *x.shape[1:]), x.dtype), [VMEM] * 4, 1, 1 << 10, out_specs=VMEM
    )(*pieces)
    for unit in (1, 4):
        a, b, c = (sent(x, lambda e, s, k=k: e ^ unit * k) for k in (1, 2, 3))
        low = lows["expert", unit]
        x = in_order(lows["expert", 2 * unit], in_order(low, x, a, 2), in_order(low, b, c, 2), 2)
    other = swap(x, "shard", CORE)
    z, chips, plane, rows = x.shape
    return call(
        router_body, jax.ShapeDtypeStruct((z * plane, chips * rows), x.dtype), [VMEM, VMEM], 2, 1 << 20, out_specs=VMEM
    )(x, other).T


def per_device(w_gate, avg_gate, w_up, avg_up, mix_share, router_weight, router_gain):
    rows, columns = w_gate.shape[1:]
    shape = (1, lax.axis_size("shard") * rows, columns)
    lows = lows_of(rows, 2 * rows)

    fresh_gate, mine = mean_of(mix_share, w_gate, avg_gate, 60, router_weight.T, router_gain[None])
    near = swap(mine, "shard", CORE)
    router = in_order(lows["shard", CORE], mine[:, columns:], near[:, columns:], 1)
    pair = jnp.concatenate([mine[:, :columns] + near[:, :columns], router], axis=1)
    totals_gate = pair, swap(pair, "shard", CHIP)
    gate = narrow(fresh_gate, totals_gate, 0, GATE[:1], False)
    *rest, whole = narrow(fresh_gate, totals_gate, GATE[0], GATE[1:], True)
    near, far = from_all([*gate, *rest], whole)
    serve_gate = place(sum(far, near), rows, shape)

    fresh_up, sums_up = mean_of(mix_share, w_up, avg_up, 56)
    pair = sums_up + swap(sums_up, "shard", CORE)
    totals_up = pair, swap(pair, "shard", CHIP)
    *up, whole, scale_up, scale_gate = narrow(fresh_up, totals_up + totals_gate, 0, UP, True, scales=2)
    near, far = from_all(up, whole)
    serve_up = place(sum(far[:2], near), rows, shape)
    serve_up = place(sum(far[2:], []), rows, shape, serve_up)

    other = totals_gate[1][:, columns:].astype(jnp.bfloat16)
    serve_router = router_of(lows, router.astype(jnp.bfloat16), other)
    return (serve_gate, serve_up, scale_gate, scale_up, serve_router)


def solution(mesh):
    return jax.shard_map(
        per_device,
        mesh=mesh,
        in_specs=(
            P("expert", "shard", None),
            P("expert", "shard", None),
            P("expert", "shard", None),
            P("expert", "shard", None),
            P("expert"),
            P("shard", "expert"),
            P("shard"),
        ),
        out_specs=(
            P("expert", None, None),
            P("expert", None, None),
            P("expert", None),
            P("expert", None),
            P(),
        ),
        check_vma=False,
    )
```

```python
import functools

import jax
import jax.numpy as jnp
from jax import lax
from jax.experimental import pallas as pl
from jax.experimental.pallas import tpu as pltpu
from jax.sharding import PartitionSpec as P


CORE, CHIP = 1, 2
GATE = (64, 192, 256)
UP = (256, 128, 112, 16)
DIRECT = 3
LOADS = 8
MIB = 1 << 20
VMEM = pl.BlockSpec(memory_space=pltpu.VMEM)
SMEM = pl.BlockSpec(memory_space=pltpu.SMEM)
HBM = pl.BlockSpec(memory_space=pltpu.HBM)


def swap(x, axis, mask):
    n = lax.axis_size(axis)
    return lax.ppermute(x, axis, [(i, i ^ mask) for i in range(n)])


def call(body, out, ins, mib, flops, **kw):
    return pl.pallas_call(
        body,
        out_shape=out,
        compiler_params=pltpu.CompilerParams(vmem_limit_bytes=mib * MIB),
        cost_estimate=pl.CostEstimate(flops=flops, bytes_accessed=4 * MIB, transcendentals=0),
        in_specs=ins,
        **kw,
    )


def mean_body(share_ref, w_ref, avg_ref, fresh_ref, sums_ref, w_buf, avg_buf, sem):
    rows = w_buf.shape[0]
    step = rows // LOADS

    def copies(k):
        at = pl.ds(k * step, step)
        return (
            pltpu.make_async_copy(w_ref.at[0, at], w_buf.at[at], sem.at[0, k]),
            pltpu.make_async_copy(avg_ref.at[0, at], avg_buf.at[at], sem.at[1, k]),
        )

    for k in range(LOADS):
        for c in copies(k):
            c.start()
    share = share_ref[0]
    rest = 1.0 - share
    total = jnp.zeros((8, w_buf.shape[1]), jnp.float32)
    for k in range(LOADS):
        for c in copies(k):
            c.wait()

        def tile(i, total):
            at = pl.ds(pl.multiple_of(k * step + i * 8, 8), 8)
            fresh = share * w_buf[at] + rest * avg_buf[at]
            fresh_ref[at] = fresh
            return total + fresh * fresh

        total = lax.fori_loop(0, step // 8, tile, total, unroll=True)
    sums_ref[...] = jnp.sum(total, axis=0, keepdims=True)


def mean_of(share, w, avg, mib):
    _, rows, columns = w.shape
    return call(
        mean_body,
        (pltpu.VMEM((rows, columns), jnp.float32), pltpu.VMEM((1, columns), jnp.float32)),
        [SMEM, HBM, HBM],
        mib,
        4 << 20,
        out_specs=(VMEM, VMEM),
        scratch_shapes=[
            pltpu.VMEM((rows, columns), jnp.float32),
            pltpu.VMEM((rows, columns), jnp.float32),
            pltpu.SemaphoreType.DMA((2, LOADS)),
        ],
    )(share, w, avg)


def narrow_body(first, blocks, whole, scales, fresh_ref, *refs):
    columns = fresh_ref.shape[1]
    totals, outs = refs[: 2 * max(scales, 1)], refs[2 * max(scales, 1) :]
    scale = [jnp.sqrt(a[:, :columns] + b[:, :columns]) for a, b in zip(totals[::2], totals[1::2])]
    inverse = 1.0 / scale[0]
    if scales:
        for value, out in zip(scale, outs[-scales:]):
            out[...] = value
        outs = outs[:-scales]

    def rows_of(at):
        return (fresh_ref[pl.ds(at, 16)] * inverse).astype(jnp.bfloat16)

    if whole:
        for at in range(0, first, 16):
            outs[-1][0, pl.ds(at, 16)] = rows_of(at)
    at = first
    for rows, out in zip(blocks, outs):
        for i in range(0, rows, 16):
            value = rows_of(at + i)
            out[0, pl.ds(i, 16)] = value
            if whole:
                outs[-1][0, pl.ds(at + i, 16)] = value
        at += rows


def narrow(fresh, totals, first, blocks, whole, scales=0):
    rows, columns = fresh.shape
    sizes = [*blocks, rows] if whole else blocks
    outs = [pltpu.VMEM((1, n, columns), jnp.bfloat16) for n in sizes]
    outs += [jax.ShapeDtypeStruct((1, columns), jnp.float32)] * scales
    return call(
        functools.partial(narrow_body, first, blocks, whole, scales),
        tuple(outs),
        [VMEM] * (1 + len(totals)),
        2,
        2 << 20,
        out_specs=(VMEM,) * len(outs),
    )(fresh, *totals)


def place_body(places, *refs):
    out, sem = refs[-2], refs[-1]
    me = lax.axis_index("shard")
    copies = []
    for k, (mask, at, rows, shard_rows) in enumerate(places):
        start = pl.multiple_of((me ^ mask) * shard_rows + at, 16)
        copies.append(pltpu.make_async_copy(refs[k].at[0], out.at[0, pl.ds(start, rows)], sem.at[k]))
    for c in copies:
        c.start()
    for c in copies:
        c.wait()


def place(pieces, shard_rows, shape, into=None):
    blocks = [p[0] for p in pieces]
    places = tuple((m, at, b.shape[1], shard_rows) for b, m, at in pieces)
    n = len(blocks)
    again = into is not None
    return call(
        functools.partial(place_body, places),
        jax.ShapeDtypeStruct(shape, blocks[0].dtype),
        [VMEM] * n + [HBM] * again,
        6,
        1 << 20,
        out_specs=HBM,
        scratch_shapes=[pltpu.SemaphoreType.DMA((n,))],
        **({"input_output_aliases": {n: 0}} if again else {}),
    )(*blocks, *([into] if again else []))


def starts(blocks):
    at, out = 0, []
    for rows in blocks:
        out.append(at)
        at += rows
    return out


def from_all(blocks, whole, direct):
    chips = [swap(b, "shard", CHIP) for b in blocks]
    boths = [swap(b, "shard", CORE) for b in chips[:direct]]
    boths += [swap(b, "shard", CORE | CHIP) for b in blocks[direct:]]
    at = starts([b.shape[1] for b in blocks])
    near = [(whole, 0, 0), (swap(whole, "shard", CORE), CORE, 0)]
    far = [[(c, CHIP, n), (b, CORE | CHIP, n)] for c, b, n in zip(chips, boths, at)]
    return near, far


BITS = (("shard", CHIP), ("expert", 1), ("expert", 2), ("expert", 4), ("expert", 8))


def lows_body(*outs):
    for (axis, mask), out in zip(BITS, outs):
        low = jnp.where((lax.axis_index(axis) & mask) == 0, 1.0, 0.0)
        out[...] = jnp.full(out.shape, low, jnp.float32)


def lows_of(rows):
    outs = call(
        lows_body,
        tuple(jax.ShapeDtypeStruct((1, rows), jnp.float32) for _ in BITS),
        [],
        1,
        1 << 10,
        out_specs=(VMEM,) * len(BITS),
    )()
    return dict(zip(BITS, outs))


def in_order(low, own, other, dim):
    low = low.reshape((1,) * (own.ndim - 2) + low.shape) > 0.5
    return jnp.concatenate([jnp.where(low, own, other), jnp.where(low, other, own)], axis=dim)


def router_body(own_ref, other_ref, out_ref):
    z, chips, plane, rows = own_ref.shape
    first = (lax.axis_index("shard") & CORE) == 0
    for k in range(z):
        for chip in range(chips):
            own, other = own_ref[k, chip], other_ref[k, chip]
            for core in range(2):
                at = (chip * 2 + core) * rows
                value = jnp.where(first, own, other) if core == 0 else jnp.where(first, other, own)
                out_ref[pl.ds(k * plane, plane), pl.ds(at, rows)] = value


def turned(x):
    experts, shards = lax.axis_size("expert"), lax.axis_size("shard")
    pairs = []
    for e in range(experts):
        for s in range(shards):
            to = (e + (16 if s & CHIP else -16)) % experts
            pairs.append((e * shards + s, to * shards + s))
    return lax.ppermute(x, ("expert", "shard"), pairs)


def planes_body(*refs):
    z = lax.axis_index("expert") // 16
    up = (lax.axis_index("shard") & CHIP) == 0
    for k, ref in enumerate(refs[:-1]):
        refs[-1][jnp.where(up, z + k, z + 4 - k) % 4] = ref[0]


def router_of(lows, own, other):
    pieces = [in_order(lows["shard", CHIP], own[None, None], other[None, None], 1)]
    for _ in range(3):
        pieces.append(turned(pieces[-1]))
    x = pieces[0]
    x = call(
        planes_body, jax.ShapeDtypeStruct((4, *x.shape[1:]), x.dtype), [VMEM] * 4, 1, 1 << 10, out_specs=VMEM
    )(*pieces)
    for unit in (1, 4):
        a, b, c = (swap(x, "expert", unit * k) for k in (1, 2, 3))
        low = lows["expert", unit]
        x = in_order(lows["expert", 2 * unit], in_order(low, x, a, 2), in_order(low, b, c, 2), 2)
    other = swap(x, "shard", CORE)
    z, chips, plane, rows = x.shape
    return call(
        router_body,
        jax.ShapeDtypeStruct((z * plane, chips * 2 * rows), x.dtype),
        [VMEM, VMEM],
        2,
        1 << 20,
        out_specs=VMEM,
    )(x, other).T


def per_device(w_gate, avg_gate, w_up, avg_up, mix_share, router_weight, router_gain):
    rows, columns = w_gate.shape[1:]
    shape = (1, lax.axis_size("shard") * rows, columns)
    part = (router_weight.T * router_gain[None]).astype(jnp.bfloat16)
    lows = lows_of(rows)

    fresh_gate, sums_gate = mean_of(mix_share, w_gate, avg_gate, 60)
    pair = sums_gate + swap(sums_gate, "shard", CORE)
    pair = jnp.concatenate([pair, part.astype(jnp.float32)], axis=1)
    totals_gate = pair, swap(pair, "shard", CHIP)
    gate = narrow(fresh_gate, totals_gate, 0, GATE[:1], False)
    *rest, whole = narrow(fresh_gate, totals_gate, GATE[0], GATE[1:], True)
    near, far = from_all([*gate, *rest], whole, len(GATE))
    serve_gate = place(sum(far, near), rows, shape)

    fresh_up, sums_up = mean_of(mix_share, w_up, avg_up, 56)
    pair = sums_up + swap(sums_up, "shard", CORE)
    totals_up = pair, swap(pair, "shard", CHIP)
    *up, whole, scale_up, scale_gate = narrow(fresh_up, totals_up + totals_gate, 0, UP, True, scales=2)
    near, far = from_all(up, whole, DIRECT)
    serve_up = place(near, rows, shape)
    serve_up = place(sum(far[:2], []), rows, shape, serve_up)
    serve_up = place(sum(far[2:], []), rows, shape, serve_up)

    other = totals_gate[1][:, columns:].astype(jnp.bfloat16)
    serve_router = router_of(lows, part, other)
    return (serve_gate, serve_up, scale_gate, scale_up, serve_router)


def solution(mesh):
    return jax.shard_map(
        per_device,
        mesh=mesh,
        in_specs=(
            P("expert", "shard", None),
            P("expert", "shard", None),
            P("expert", "shard", None),
            P("expert", "shard", None),
            P("expert"),
            P("shard", "expert"),
            P("shard"),
        ),
        out_specs=(
            P("expert", None, None),
            P("expert", None, None),
            P("expert", None),
            P("expert", None),
            P(),
        ),
        check_vma=False,
    )
```

```python
import functools

import jax
import jax.numpy as jnp
from jax import lax
from jax.experimental import pallas as pl
from jax.experimental.pallas import tpu as pltpu
from jax.sharding import PartitionSpec as P


CORE, CHIP = 1, 2
GATE = (112, 144, 256)
UP = (256, 128, 64, 64)
LOADS = 8
MIB = 1 << 20
VMEM = pl.BlockSpec(memory_space=pltpu.VMEM)
SMEM = pl.BlockSpec(memory_space=pltpu.SMEM)
HBM = pl.BlockSpec(memory_space=pltpu.HBM)


def swap(x, axis, mask):
    n = lax.axis_size(axis)
    return lax.ppermute(x, axis, [(i, i ^ mask) for i in range(n)])


def call(body, out, ins, mib, flops, **kw):
    return pl.pallas_call(
        body,
        out_shape=out,
        compiler_params=pltpu.CompilerParams(vmem_limit_bytes=mib * MIB),
        cost_estimate=pl.CostEstimate(flops=flops, bytes_accessed=4 * MIB, transcendentals=0),
        in_specs=ins,
        **kw,
    )


def mean_body(first, share_ref, w_ref, avg_ref, fresh_ref, sums_ref, w_buf, avg_buf, sem):
    rows = w_buf.shape[0]
    step = rows // LOADS

    def copies(k):
        at, source = pl.ds(k * step, step), pl.ds(first + k * step, step)
        return (
            pltpu.make_async_copy(w_ref.at[0, source], w_buf.at[at], sem.at[0, k]),
            pltpu.make_async_copy(avg_ref.at[0, source], avg_buf.at[at], sem.at[1, k]),
        )

    for k in range(LOADS):
        for c in copies(k):
            c.start()
    share = share_ref[0]
    rest = 1.0 - share
    total = jnp.zeros((8, w_buf.shape[1]), jnp.float32)
    for k in range(LOADS):
        for c in copies(k):
            c.wait()

        def tile(i, total):
            at = pl.ds(pl.multiple_of(k * step + i * 8, 8), 8)
            fresh = share * w_buf[at] + rest * avg_buf[at]
            fresh_ref[at] = fresh
            return total + fresh * fresh

        total = lax.fori_loop(0, step // 8, tile, total, unroll=True)
    sums_ref[...] = jnp.sum(total, axis=0, keepdims=True)


def mean_of(share, w, avg, mib, first=0, rows=None):
    columns = w.shape[2]
    rows = rows or w.shape[1]
    return call(
        functools.partial(mean_body, first),
        (pltpu.VMEM((rows, columns), jnp.float32), pltpu.VMEM((1, columns), jnp.float32)),
        [SMEM, HBM, HBM],
        mib,
        4 << 20,
        out_specs=(VMEM, VMEM),
        scratch_shapes=[
            pltpu.VMEM((rows, columns), jnp.float32),
            pltpu.VMEM((rows, columns), jnp.float32),
            pltpu.SemaphoreType.DMA((2, LOADS)),
        ],
    )(share, w, avg)


def narrow_body(first, blocks, whole, scales, parts, *refs):
    fresh, refs = refs[:parts], refs[parts:]
    part_rows, columns = fresh[0].shape
    totals, outs = refs[: 2 * max(scales, 1)], refs[2 * max(scales, 1) :]
    scale = [jnp.sqrt(a[:, :columns] + b[:, :columns]) for a, b in zip(totals[::2], totals[1::2])]
    inverse = 1.0 / scale[0]
    if scales:
        for value, out in zip(scale, outs[-scales:]):
            out[...] = value
        outs = outs[:-scales]

    def rows_of(at):
        return (fresh[at // part_rows][pl.ds(at % part_rows, 16)] * inverse).astype(jnp.bfloat16)

    if whole:
        for at in range(0, first, 16):
            outs[-1][0, pl.ds(at, 16)] = rows_of(at)
    at = first
    for rows, out in zip(blocks, outs):
        for i in range(0, rows, 16):
            value = rows_of(at + i)
            out[0, pl.ds(i, 16)] = value
            if whole:
                outs[-1][0, pl.ds(at + i, 16)] = value
        at += rows


def narrow(fresh, totals, first, blocks, whole, scales=0):
    rows, columns = sum(f.shape[0] for f in fresh), fresh[0].shape[1]
    sizes = [*blocks, rows] if whole else blocks
    outs = [pltpu.VMEM((1, n, columns), jnp.bfloat16) for n in sizes]
    outs += [jax.ShapeDtypeStruct((1, columns), jnp.float32)] * scales
    return call(
        functools.partial(narrow_body, first, blocks, whole, scales, len(fresh)),
        tuple(outs),
        [VMEM] * (len(fresh) + len(totals)),
        2,
        2 << 20,
        out_specs=(VMEM,) * len(outs),
    )(*fresh, *totals)


def place_body(places, *refs):
    out, sem = refs[-2], refs[-1]
    me = lax.axis_index("shard")
    copies = []
    for k, (mask, at, rows, shard_rows) in enumerate(places):
        start = pl.multiple_of((me ^ mask) * shard_rows + at, 16)
        copies.append(pltpu.make_async_copy(refs[k].at[0], out.at[0, pl.ds(start, rows)], sem.at[k]))
    for c in copies:
        c.start()
    for c in copies:
        c.wait()


def place(pieces, shard_rows, shape, into=None):
    blocks = [p[0] for p in pieces]
    places = tuple((m, at, b.shape[1], shard_rows) for b, m, at in pieces)
    n = len(blocks)
    again = into is not None
    return call(
        functools.partial(place_body, places),
        jax.ShapeDtypeStruct(shape, blocks[0].dtype),
        [VMEM] * n + [HBM] * again,
        6,
        1 << 20,
        out_specs=HBM,
        scratch_shapes=[pltpu.SemaphoreType.DMA((n,))],
        **({"input_output_aliases": {n: 0}} if again else {}),
    )(*blocks, *([into] if again else []))


def starts(blocks):
    at, out = 0, []
    for rows in blocks:
        out.append(at)
        at += rows
    return out


def from_all(blocks, whole):
    chips = [swap(b, "shard", CHIP) for b in blocks]
    boths = [swap(b, "shard", CORE) for b in chips]
    at = starts([b.shape[1] for b in blocks])
    near = [(whole, 0, 0), (swap(whole, "shard", CORE), CORE, 0)]
    far = [[(c, CHIP, n), (b, CORE | CHIP, n)] for c, b, n in zip(chips, boths, at)]
    return near, far


BITS = (("shard", CHIP), ("expert", 1), ("expert", 2), ("expert", 4), ("expert", 8))


def lows_body(*outs):
    for (axis, mask), out in zip(BITS, outs):
        low = jnp.where((lax.axis_index(axis) & mask) == 0, 1.0, 0.0)
        out[...] = jnp.full(out.shape, low, jnp.float32)


def lows_of(rows):
    outs = call(
        lows_body,
        tuple(jax.ShapeDtypeStruct((1, rows), jnp.float32) for _ in BITS),
        [],
        1,
        1 << 10,
        out_specs=(VMEM,) * len(BITS),
    )()
    return dict(zip(BITS, outs))


def in_order(low, own, other, dim):
    low = low.reshape((1,) * (own.ndim - 2) + low.shape) > 0.5
    return jnp.concatenate([jnp.where(low, own, other), jnp.where(low, other, own)], axis=dim)


def router_body(own_ref, other_ref, out_ref):
    z, chips, plane, rows = own_ref.shape
    first = (lax.axis_index("shard") & CORE) == 0
    for k in range(z):
        for chip in range(chips):
            own, other = own_ref[k, chip], other_ref[k, chip]
            for core in range(2):
                at = (chip * 2 + core) * rows
                value = jnp.where(first, own, other) if core == 0 else jnp.where(first, other, own)
                out_ref[pl.ds(k * plane, plane), pl.ds(at, rows)] = value


def turned(x):
    experts, shards = lax.axis_size("expert"), lax.axis_size("shard")
    pairs = []
    for e in range(experts):
        for s in range(shards):
            to = (e + (16 if s & CHIP else -16)) % experts
            pairs.append((e * shards + s, to * shards + s))
    return lax.ppermute(x, ("expert", "shard"), pairs)


def planes_body(*refs):
    z = lax.axis_index("expert") // 16
    up = (lax.axis_index("shard") & CHIP) == 0
    for k, ref in enumerate(refs[:-1]):
        refs[-1][jnp.where(up, z + k, z + 4 - k) % 4] = ref[0]


def router_of(lows, own, other):
    pieces = [in_order(lows["shard", CHIP], own[None, None], other[None, None], 1)]
    for _ in range(3):
        pieces.append(turned(pieces[-1]))
    x = pieces[0]
    x = call(
        planes_body,
        jax.ShapeDtypeStruct((4, *x.shape[1:]), x.dtype),
        [VMEM] * 4,
        1,
        1 << 10,
        out_specs=VMEM,
    )(*pieces)
    for unit in (1, 4):
        a, b, c = (swap(x, "expert", unit * k) for k in (1, 2, 3))
        low = lows["expert", unit]
        x = in_order(lows["expert", 2 * unit], in_order(low, x, a, 2), in_order(low, b, c, 2), 2)
    other = swap(x, "shard", CORE)
    z, chips, plane, rows = x.shape
    return call(
        router_body,
        jax.ShapeDtypeStruct((z * plane, chips * 2 * rows), x.dtype),
        [VMEM, VMEM],
        2,
        1 << 20,
        out_specs=VMEM,
    )(x, other).T


def per_device(w_gate, avg_gate, w_up, avg_up, mix_share, router_weight, router_gain):
    rows, columns = w_gate.shape[1:]
    shape = (1, lax.axis_size("shard") * rows, columns)
    part = (router_weight.T * router_gain[None]).astype(jnp.bfloat16)
    lows = lows_of(rows)

    fresh_gate, sums_gate = mean_of(mix_share, w_gate, avg_gate, 60)
    pair = sums_gate + swap(sums_gate, "shard", CORE)
    pair = jnp.concatenate([pair, part.astype(jnp.float32)], axis=1)
    totals_gate = pair, swap(pair, "shard", CHIP)
    gate = narrow([fresh_gate], totals_gate, 0, GATE[:1], False)
    *rest, whole = narrow([fresh_gate], totals_gate, GATE[0], GATE[1:], True)
    near, far = from_all([*gate, *rest], whole)
    serve_gate = place(sum(far, near), rows, shape)

    half = rows // 2
    fresh_0, sums_0 = mean_of(mix_share, w_up, avg_up, 58, 0, half)
    fresh_1, sums_1 = mean_of(mix_share, w_up, avg_up, 56, half, half)
    fresh_up, sums_up = [fresh_0, fresh_1], sums_0 + sums_1
    pair = sums_up + swap(sums_up, "shard", CORE)
    totals_up = pair, swap(pair, "shard", CHIP)
    *up, whole, scale_up, scale_gate = narrow(
        fresh_up, totals_up + totals_gate, 0, UP, True, scales=2
    )
    near, far = from_all(up, whole)
    serve_up = place(near, rows, shape)
    serve_up = place(sum(far[:2], []), rows, shape, serve_up)
    serve_up = place(sum(far[2:], []), rows, shape, serve_up)

    other = totals_gate[1][:, columns:].astype(jnp.bfloat16)
    serve_router = router_of(lows, part, other)
    return (serve_gate, serve_up, scale_gate, scale_up, serve_router)


def solution(mesh):
    return jax.shard_map(
        per_device,
        mesh=mesh,
        in_specs=(
            P("expert", "shard", None),
            P("expert", "shard", None),
            P("expert", "shard", None),
            P("expert", "shard", None),
            P("expert"),
            P("shard", "expert"),
            P("shard"),
        ),
        out_specs=(
            P("expert", None, None),
            P("expert", None, None),
            P("expert", None),
            P("expert", None),
            P(),
        ),
        check_vma=False,
    )
```

```python
import functools

import jax
import jax.numpy as jnp
from jax import lax
from jax.experimental import pallas as pl
from jax.experimental.pallas import tpu as pltpu
from jax.sharding import PartitionSpec as P


CORE, CHIP = 1, 2
GATE = (64, 192, 256)
UP = (256, 128, 64, 64)
LOADS = 8
MIB = 1 << 20
VMEM = pl.BlockSpec(memory_space=pltpu.VMEM)
SMEM = pl.BlockSpec(memory_space=pltpu.SMEM)
HBM = pl.BlockSpec(memory_space=pltpu.HBM)


def swap(x, axis, mask):
    n = lax.axis_size(axis)
    return lax.ppermute(x, axis, [(i, i ^ mask) for i in range(n)])


def call(body, out, ins, mib, flops, **kw):
    return pl.pallas_call(
        body,
        out_shape=out,
        compiler_params=pltpu.CompilerParams(vmem_limit_bytes=mib * MIB),
        cost_estimate=pl.CostEstimate(flops=flops, bytes_accessed=4 * MIB, transcendentals=0),
        in_specs=ins,
        **kw,
    )


def mean_body(share_ref, w_ref, avg_ref, fresh_ref, sums_ref, w_buf, avg_buf, sem):
    rows = w_buf.shape[0]
    step = rows // LOADS

    def copies(k):
        at = pl.ds(k * step, step)
        return (
            pltpu.make_async_copy(w_ref.at[0, at], w_buf.at[at], sem.at[0, k]),
            pltpu.make_async_copy(avg_ref.at[0, at], avg_buf.at[at], sem.at[1, k]),
        )

    for k in range(LOADS):
        for c in copies(k):
            c.start()
    share = share_ref[0]
    rest = 1.0 - share
    total = jnp.zeros((8, w_buf.shape[1]), jnp.float32)
    for k in range(LOADS):
        for c in copies(k):
            c.wait()

        def tile(i, total):
            at = pl.ds(pl.multiple_of(k * step + i * 8, 8), 8)
            fresh = share * w_buf[at] + rest * avg_buf[at]
            fresh_ref[at] = fresh
            return total + fresh * fresh

        total = lax.fori_loop(0, step // 8, tile, total, unroll=True)
    sums_ref[...] = jnp.sum(total, axis=0, keepdims=True)


def mean_of(share, w, avg, mib):
    _, rows, columns = w.shape
    return call(
        mean_body,
        (pltpu.VMEM((rows, columns), jnp.float32), pltpu.VMEM((1, columns), jnp.float32)),
        [SMEM, HBM, HBM],
        mib,
        4 << 20,
        out_specs=(VMEM, VMEM),
        scratch_shapes=[
            pltpu.VMEM((rows, columns), jnp.float32),
            pltpu.VMEM((rows, columns), jnp.float32),
            pltpu.SemaphoreType.DMA((2, LOADS)),
        ],
    )(share, w, avg)


def narrow_body(first, blocks, whole, scales, fresh_ref, *refs):
    columns = fresh_ref.shape[1]
    totals, outs = refs[: 2 * max(scales, 1)], refs[2 * max(scales, 1) :]
    scale = [jnp.sqrt(a[:, :columns] + b[:, :columns]) for a, b in zip(totals[::2], totals[1::2])]
    inverse = 1.0 / scale[0]
    if scales:
        for value, out in zip(scale, outs[-scales:]):
            out[...] = value
        outs = outs[:-scales]

    def rows_of(at):
        return (fresh_ref[pl.ds(at, 16)] * inverse).astype(jnp.bfloat16)

    if whole:
        for at in range(0, first, 16):
            outs[-1][0, pl.ds(at, 16)] = rows_of(at)
    at = first
    for rows, out in zip(blocks, outs):
        for i in range(0, rows, 16):
            value = rows_of(at + i)
            out[0, pl.ds(i, 16)] = value
            if whole:
                outs[-1][0, pl.ds(at + i, 16)] = value
        at += rows


def narrow(fresh, totals, first, blocks, whole, scales=0):
    rows, columns = fresh.shape
    sizes = [*blocks, rows] if whole else blocks
    outs = [pltpu.VMEM((1, n, columns), jnp.bfloat16) for n in sizes]
    outs += [jax.ShapeDtypeStruct((1, columns), jnp.float32)] * scales
    return call(
        functools.partial(narrow_body, first, blocks, whole, scales),
        tuple(outs),
        [VMEM] * (1 + len(totals)),
        2,
        2 << 20,
        out_specs=(VMEM,) * len(outs),
    )(fresh, *totals)


def place_body(places, *refs):
    out, sem = refs[-2], refs[-1]
    me = lax.axis_index("shard")
    copies = []
    for k, (mask, at, rows, shard_rows) in enumerate(places):
        start = pl.multiple_of((me ^ mask) * shard_rows + at, 16)
        copies.append(pltpu.make_async_copy(refs[k].at[0], out.at[0, pl.ds(start, rows)], sem.at[k]))
    for c in copies:
        c.start()
    for c in copies:
        c.wait()


def place(pieces, shard_rows, shape, into=None):
    blocks = [p[0] for p in pieces]
    places = tuple((m, at, b.shape[1], shard_rows) for b, m, at in pieces)
    n = len(blocks)
    again = into is not None
    return call(
        functools.partial(place_body, places),
        jax.ShapeDtypeStruct(shape, blocks[0].dtype),
        [VMEM] * n + [HBM] * again,
        6,
        1 << 20,
        out_specs=HBM,
        scratch_shapes=[pltpu.SemaphoreType.DMA((n,))],
        **({"input_output_aliases": {n: 0}} if again else {}),
    )(*blocks, *([into] if again else []))


def starts(blocks):
    at, out = 0, []
    for rows in blocks:
        out.append(at)
        at += rows
    return out


def from_all(blocks, whole):
    chips = [swap(b, "shard", CHIP) for b in blocks]
    boths = [swap(b, "shard", CORE) for b in chips]
    at = starts([b.shape[1] for b in blocks])
    near = [(whole, 0, 0), (swap(whole, "shard", CORE), CORE, 0)]
    far = [[(c, CHIP, n), (b, CORE | CHIP, n)] for c, b, n in zip(chips, boths, at)]
    return near, far


BITS = (("shard", CHIP), ("expert", 1), ("expert", 2), ("expert", 4), ("expert", 8))


def lows_body(*outs):
    for (axis, mask), out in zip(BITS, outs):
        low = jnp.where((lax.axis_index(axis) & mask) == 0, 1.0, 0.0)
        out[...] = jnp.full(out.shape, low, jnp.float32)


def lows_of(rows):
    outs = call(
        lows_body,
        tuple(jax.ShapeDtypeStruct((1, rows), jnp.float32) for _ in BITS),
        [],
        1,
        1 << 10,
        out_specs=(VMEM,) * len(BITS),
    )()
    return dict(zip(BITS, outs))


def in_order(low, own, other, dim):
    low = low.reshape((1,) * (own.ndim - 2) + low.shape) > 0.5
    return jnp.concatenate([jnp.where(low, own, other), jnp.where(low, other, own)], axis=dim)


def router_body(own_ref, other_ref, out_ref):
    z, chips, plane, rows = own_ref.shape
    first = (lax.axis_index("shard") & CORE) == 0
    for k in range(z):
        for chip in range(chips):
            own, other = own_ref[k, chip], other_ref[k, chip]
            for core in range(2):
                at = (chip * 2 + core) * rows
                value = jnp.where(first, own, other) if core == 0 else jnp.where(first, other, own)
                out_ref[pl.ds(k * plane, plane), pl.ds(at, rows)] = value


def turned(x):
    experts, shards = lax.axis_size("expert"), lax.axis_size("shard")
    pairs = []
    for e in range(experts):
        for s in range(shards):
            to = (e + (16 if s & CHIP else -16)) % experts
            pairs.append((e * shards + s, to * shards + s))
    return lax.ppermute(x, ("expert", "shard"), pairs)


def planes_body(*refs):
    z = lax.axis_index("expert") // 16
    up = (lax.axis_index("shard") & CHIP) == 0
    for k, ref in enumerate(refs[:-1]):
        refs[-1][jnp.where(up, z + k, z + 4 - k) % 4] = ref[0]


def router_of(lows, own, other):
    pieces = [in_order(lows["shard", CHIP], own[None, None], other[None, None], 1)]
    for _ in range(3):
        pieces.append(turned(pieces[-1]))
    x = pieces[0]
    x = call(
        planes_body,
        jax.ShapeDtypeStruct((4, *x.shape[1:]), x.dtype),
        [VMEM] * 4,
        1,
        1 << 10,
        out_specs=VMEM,
    )(*pieces)
    for unit in (1, 4):
        a, b, c = (swap(x, "expert", unit * k) for k in (1, 2, 3))
        low = lows["expert", unit]
        x = in_order(lows["expert", 2 * unit], in_order(low, x, a, 2), in_order(low, b, c, 2), 2)
    other = swap(x, "shard", CORE)
    z, chips, plane, rows = x.shape
    return call(
        router_body,
        jax.ShapeDtypeStruct((z * plane, chips * 2 * rows), x.dtype),
        [VMEM, VMEM],
        2,
        1 << 20,
        out_specs=VMEM,
    )(x, other).T


def per_device(w_gate, avg_gate, w_up, avg_up, mix_share, router_weight, router_gain):
    rows, columns = w_gate.shape[1:]
    shape = (1, lax.axis_size("shard") * rows, columns)
    part = (router_weight.T * router_gain[None]).astype(jnp.bfloat16)
    lows = lows_of(rows)

    fresh_gate, sums_gate = mean_of(mix_share, w_gate, avg_gate, 60)
    pair = sums_gate + swap(sums_gate, "shard", CORE)
    pair = jnp.concatenate([pair, part.astype(jnp.float32)], axis=1)
    totals_gate = pair, swap(pair, "shard", CHIP)
    gate = narrow(fresh_gate, totals_gate, 0, GATE[:1], False)
    *rest, whole = narrow(fresh_gate, totals_gate, GATE[0], GATE[1:], True)
    near, far = from_all([*gate, *rest], whole)
    serve_gate = place(sum(far, near), rows, shape)

    fresh_up, sums_up = mean_of(mix_share, w_up, avg_up, 56)
    pair = sums_up + swap(sums_up, "shard", CORE)
    totals_up = pair, swap(pair, "shard", CHIP)
    *up, whole, scale_up, scale_gate = narrow(
        fresh_up, totals_up + totals_gate, 0, UP, True, scales=2
    )
    near, far = from_all(up, whole)
    serve_up = place(near, rows, shape)
    serve_up = place(sum(far[:2], []), rows, shape, serve_up)
    serve_up = place(sum(far[2:], []), rows, shape, serve_up)

    other = totals_gate[1][:, columns:].astype(jnp.bfloat16)
    serve_router = router_of(lows, part, other)
    return (serve_gate, serve_up, scale_gate, scale_up, serve_router)


def solution(mesh):
    return jax.shard_map(
        per_device,
        mesh=mesh,
        in_specs=(
            P("expert", "shard", None),
            P("expert", "shard", None),
            P("expert", "shard", None),
            P("expert", "shard", None),
            P("expert"),
            P("shard", "expert"),
            P("shard"),
        ),
        out_specs=(
            P("expert", None, None),
            P("expert", None, None),
            P("expert", None),
            P("expert", None),
            P(),
        ),
        check_vma=False,
    )
```
